32 devices in a mesh: parts: 2 (over x), seq: 16 (over z, y, core).
Axes of the slice: x: 2, y: 2, z: 4, core: 2. Of those that a mesh axis runs over, the one named last changes fastest.
Arguments:
- queries: bfloat16 [3072, 1024], P(('parts', 'seq')), parts along dimension 0, may hold values from -8 to 8
- self_keys: bfloat16 [3072, 1024], P(('parts', 'seq')), parts along dimension 0, may hold values from -8 to 8
- self_values: bfloat16 [3072, 1024], P(('parts', 'seq')), parts along dimension 0, may hold values from -8 to 8
- residual_in: bfloat16 [3072, 1024], P(('parts', 'seq')), parts along dimension 0, may hold values from -0.23925781 to 0.23925781
- text_keys: bfloat16 [2, 8, 256, 1024], P(None, 'parts', None, 'seq'), parts along dimension 1, may hold values from -8 to 8
- text_values: bfloat16 [2, 8, 256, 1024], P(None, 'parts', None, 'seq'), parts along dimension 1, may hold values from -8 to 8
- text_lengths: int32 [2, 8], P(None, 'parts'), parts along dimension 1, may hold values from 2 to 256
- frame_counts: int32 [8], P('parts'), parts along dimension 0, may hold values from 1 to 16, 24 in all
- mod_gain: float32 [1024], replicated, may hold values from 0.1 to 1.9
- mod_shift: float32 [1024], replicated, may hold values from -1.8 to 1.8
- head_weight: bfloat16 [1024, 64], replicated, may hold values from -0.1875 to 0.1875
- head_bias: float32 [64], replicated, may hold values from -1.8 to 1.8
- guide_scale: float32 [1], replicated, may hold values from 3 to 7
Outputs:
- guided: float32 [1536, 64], P(('parts', 'seq')), parts along dimension 0
The draws below stay inside these ranges and needn't reach their ends.
There are 2 independent parts, one for each index of `parts`. The reference program is written for one: setup_inputs(seed, part) draws one part's arguments, and reference() takes and returns one part's arrays. A program takes and returns all parts, laid end to end along the dimension named above; an argument that names none is the same for every part. Nothing has to cross between parts.
Inputs may be any that keep to these rules, and one draw needn't show every extreme that they name: `frame_counts`: latent frames of the 4 videos in packing order; they sum to 24 and the largest is exactly 16. `text_lengths`: live prompt tokens, counted from the front of each prompt.
All inputs are finite; a program needn't handle non-finite values.
Results may differ from the reference program's by a relative error of at most 0.0049.
Values may be sent and summed in bfloat16 or wider, within the bound.
No kernel may reach another device: no remote copies, remote signals or barrier semaphores. Data moves between devices by JAX's collectives and lax.ppermute only.
A program may use at most 64 MiB of HBM per device.

```python
import math
import jax
import jax.numpy as jnp
import numpy as np
from jax import lax

HEAD_CHANNELS = 128
HEADS = 8
D = 1024
OUT = 64
TOK_DEV = 96
TPF = 32
TEXT = 256
VIDEOS = 4
TOKENS = 768
LATENT_FRAMES = 24
MAX_FRAMES = 16


def clipped_normal(key, shape):
    return jnp.clip(jax.random.normal(key, shape, jnp.float32), -8.0, 8.0)


def draw_queries(key, part):
    value_rows = clipped_normal(jax.random.fold_in(key, 11), (2 * TOKENS, D))
    return value_rows.astype(jnp.bfloat16)


def draw_self_keys(key, part):
    value_rows = clipped_normal(jax.random.fold_in(key, 12), (2 * TOKENS, D))
    return value_rows.astype(jnp.bfloat16)


def draw_text_keys(key, part):
    value_rows = clipped_normal(jax.random.fold_in(key, 13), (2, VIDEOS, TEXT, D))
    return value_rows.astype(jnp.bfloat16)


def with_ends(values, rng, least, top_value):
    dims = values.shape
    index_at = [jax.random.randint(jax.random.fold_in(rng, axis), (), 0, dims[axis]) for axis in range(len(dims))]
    values = values.at[tuple(index_at)].set(least)
    longest = dims.index(max(dims))
    index_at[longest] = (index_at[longest] + 1) % dims[longest]
    return values.at[tuple(index_at)].set(top_value)


def level_of(own_key, shape, shards, smallest, high):
    def one(dim, shards_of):
        heights = jax.random.uniform(jax.random.fold_in(jax.random.fold_in(own_key, 6), dim), (shards_of,), jnp.float32, smallest / len(shards), high / len(shards))
        return jnp.repeat(jnp.exp(heights), shape[dim] // shards_of).reshape((-1,) + (1,) * (len(shape) - dim - 1))

    loudness = one(*shards[0])
    for cut in shards[1:]:
        loudness = loudness * one(*cut)
    return loudness


def split_up(number_of, total, limit, slope):
    weights = [(1 << 20) // math.isqrt(rank ** slope) + 1 for rank in range(2, number_of + 1)]
    spare, counts = total - limit - (number_of - 1), [1] * (number_of - 1)
    while spare > 0:
        movable = [i for i in range(number_of - 1) if counts[i] < limit]
        mass, budget = sum([weights[i] for i in movable]), spare
        for i in movable:
            more = min(limit - counts[i], max(1, budget * weights[i] // mass), spare)
            counts[i] = counts[i] + more
            spare = spare - more
    return np.array([limit] + counts)


def ragged_sizes(rng, amount, total, reach, lean):
    if amount == 2:
        one = jax.random.randint(rng, (), max(1, total - reach), min(reach, total - 1) + 1)
        return jnp.stack([one, total - one])
    lengths = jnp.asarray(split_up(amount, total, reach, lean), jnp.int32)
    couples = (amount - 1) // 2
    source_of, sink = lengths[1:1 + 2 * couples:2], lengths[2:2 + 2 * couples:2]
    margin = jnp.minimum(source_of - 1, reach - sink)
    passed = jax.random.randint(jax.random.fold_in(rng, 1), (couples,), 0, 1 << 20) % (margin + 1)
    lengths = lengths.at[1:1 + 2 * couples:2].set(source_of - passed).at[2:2 + 2 * couples:2].set(sink + passed)
    return lengths[jax.random.permutation(jax.random.fold_in(rng, 2), amount)]


def gaussian(stream_key, shape, scale, limit, shards=(), kind=jnp.bfloat16):
    drawn = jax.random.normal(stream_key, shape, jnp.float32) * scale
    if len(shards) > 0:
        drawn = level_of(stream_key, shape, shards, -0.22, 0.18) * drawn
    return jnp.clip(drawn, min=-limit, max=limit).astype(kind)


def setup_inputs(seed: int = 0, part: int = 0) -> dict:
    key_list = jax.random.split(jax.random.key(seed), 14)
    part_splits = jax.random.split(jax.random.fold_in(key_list[13], part), 14)
    queries = draw_queries(jax.random.fold_in(jax.random.fold_in(key_list[13], part), 71), part)
    self_keys = draw_self_keys(jax.random.fold_in(jax.random.fold_in(key_list[13], part), 71), part)
    self_values = gaussian(part_splits[2], (2 * TOKENS, D), 1.0, 8.0, ((0, 16),))
    residual_in = gaussian(part_splits[3], (2 * TOKENS, D), 0.03, 0.23925781, ((0, 16),))
    text_keys = draw_text_keys(jax.random.fold_in(jax.random.fold_in(key_list[13], part), 71), part)
    text_values = gaussian(part_splits[5], (2, VIDEOS, TEXT, D), 1.0, 8.0, ((3, 16),))
    text_lengths = with_ends(jax.random.randint(part_splits[6], (2, VIDEOS), 2, TEXT + 1), jax.random.fold_in(part_splits[6], 1), 2, TEXT).astype(jnp.int32)
    frame_counts = ragged_sizes(part_splits[7], VIDEOS, LATENT_FRAMES, MAX_FRAMES, 2).astype(jnp.int32)
    mod_gain = jnp.clip(1.0 + 0.18 * jax.random.normal(key_list[8], (D,), jnp.float32), 0.1, 1.9)
    mod_shift = gaussian(key_list[9], (D,), 0.3, 1.8, (), jnp.float32)
    head_weight = gaussian(key_list[10], (D, OUT), D ** -0.5, 0.1875)
    head_bias = gaussian(key_list[11], (OUT,), 0.3, 1.8, (), jnp.float32)
    guide_scale = jnp.clip(jax.random.uniform(key_list[12], (1,), jnp.float32, 3.0, 7.0), 3.0, 7.0)
    return {"queries": queries, "self_keys": self_keys, "self_values": self_values, "residual_in": residual_in, "text_keys": text_keys, "text_values": text_values, "text_lengths": text_lengths, "frame_counts": frame_counts, "mod_gain": mod_gain, "mod_shift": mod_shift, "head_weight": head_weight, "head_bias": head_bias, "guide_scale": guide_scale}


def branch_major(packed):
    features = packed.shape[1]
    device_slices = packed.shape[0] // (2 * TOK_DEV)
    grouped = packed.reshape(device_slices, 2, TOK_DEV, features)
    return grouped.transpose(1, 0, 2, 3).reshape(2, device_slices * TOK_DEV, features)

def by_heads(arranged):
    return arranged.reshape(2, arranged.shape[1], HEADS, HEAD_CHANNELS).transpose(2, 0, 1, 3)

def soft_attend(queries, incoming_keys, value_rows, allowed):
    logit_scores = jnp.einsum('pag,pmg->pam', queries.astype(jnp.float32), incoming_keys.astype(jnp.float32)) * HEAD_CHANNELS ** (-0.5)
    logit_scores = jnp.where(allowed, logit_scores, -1e+30)
    row_max = lax.optimization_barrier(jnp.max(logit_scores, axis=-1, keepdims=True))
    raised = jnp.exp(logit_scores - row_max)
    softmax_weights = (raised / lax.optimization_barrier(jnp.sum(raised, axis=-1, keepdims=True))).astype(jnp.bfloat16)
    return jnp.einsum('ehm,emp->ehp', softmax_weights.astype(jnp.float32), value_rows.astype(jnp.float32))

def reference(queries, self_keys, self_values, residual_in, text_keys, text_values, text_lengths, frame_counts, mod_gain, mod_shift, head_weight, head_bias, guide_scale):
    video_ends = jnp.cumsum(frame_counts.astype(jnp.int32)) * TPF
    positions = jnp.arange(TOKENS, dtype=jnp.int32)
    video_ids = lax.optimization_barrier(jnp.sum((positions[:, None] >= video_ends[None, :]).astype(jnp.int32), axis=1))
    self_allowed = (video_ids[:, None] == video_ids[None, :])[None]
    text_slots = jnp.arange(VIDEOS * TEXT, dtype=jnp.int32)
    slot_video = text_slots // TEXT
    slot_place = text_slots % TEXT
    live_slot = slot_place[None, :] < text_lengths.astype(jnp.int32)[:, slot_video]
    cross_allowed = (video_ids[None, :, None] == slot_video[None, None, :]) & live_slot[:, None, :]
    operands = (by_heads(branch_major(queries)), by_heads(branch_major(self_keys)), by_heads(branch_major(self_values)), by_heads(text_keys.reshape(2, VIDEOS * TEXT, D)), by_heads(text_values.reshape(2, VIDEOS * TEXT, D)))

    def per_head(pieces):
        head_query, head_key, head_value, head_tkey, head_tvalue = pieces
        combined = soft_attend(head_query, head_key, head_value, self_allowed) + soft_attend(head_query, head_tkey, head_tvalue, cross_allowed)
        return combined.astype(jnp.bfloat16)
    attention = lax.map(per_head, operands)
    attention = attention.transpose(1, 2, 0, 3).reshape(2, TOKENS, D)
    hidden = branch_major(residual_in).astype(jnp.float32) + attention.astype(jnp.float32)
    row_mean = lax.optimization_barrier(jnp.mean(hidden, axis=-1, keepdims=True))
    centred = hidden - row_mean
    row_var = lax.optimization_barrier(jnp.mean(centred * centred, axis=-1, keepdims=True))
    normed = (centred * lax.rsqrt(row_var + 1e-06) * mod_gain + mod_shift).astype(jnp.bfloat16)
    velocity = jnp.dot(normed.reshape(2 * TOKENS, D), head_weight, preferred_element_type=jnp.float32).reshape(2, TOKENS, OUT) + head_bias
    return velocity[1] + guide_scale[0] * (velocity[0] - velocity[1])
```

```python
import functools
import math

import jax
import jax.numpy as jnp
from jax import lax
from jax.experimental import pallas as pl
from jax.experimental.pallas import tpu as pltpu
from jax.sharding import PartitionSpec as P

HEAD_CHANNELS = 128
TPF = 32
CHUNK = 4 * TPF
SCALE = HEAD_CHANNELS ** (-0.5)
LOG2E = math.log2(math.e)
UNROLL_CHIPS = 8


VMEM = pl.BlockSpec(memory_space=pltpu.VMEM)
SMEM = pl.BlockSpec(memory_space=pltpu.SMEM)
ANY = pl.BlockSpec(memory_space=pl.ANY)


def chip_pairs(devices, k):
    return [(source, source ^ (2 * k)) for source in range(devices)]


def core_pairs(devices):
    return [(source, source ^ 1) for source in range(devices)]


def my_chip():
    return lax.axis_index("seq") // 2


def my_core():
    return lax.axis_index("seq") % 2


def rows(start, size):
    return pl.ds(pl.multiple_of(start, TPF), size)


def pack_kernel(chips, q_ref, k_ref, v_ref, *rest):
    q_outs, kv_outs, sems = rest[:chips], rest[chips : 2 * chips], rest[2 * chips]
    tok = q_ref.shape[0]
    chip = my_chip()
    copies = []
    for k in range(chips):
        cols = pl.ds(pl.multiple_of((chip ^ k) * HEAD_CHANNELS, HEAD_CHANNELS), HEAD_CHANNELS)
        for source, target in (
            (q_ref, q_outs[k]),
            (k_ref, kv_outs[k].at[pl.ds(0, tok)]),
            (v_ref, kv_outs[k].at[pl.ds(tok, tok)]),
        ):
            copies.append(pltpu.make_async_copy(source.at[:, cols], target, sems.at[len(copies)]))
    for copy in copies:
        copy.start()
    for copy in copies:
        copy.wait()


def softmax_parts(scores):
    top = jnp.max(scores, axis=-1, keepdims=True)
    raised = jnp.exp2((scores - top) * (SCALE * LOG2E))
    return raised, jnp.sum(raised, axis=-1, keepdims=True)


def cross_kernel(chips, counts_ref, lengths_ref, tk_own, tv_own, tk_other, tv_other, *rest):
    q_refs, out_ref = rest[:chips], rest[chips]
    qs, tk, tv = rest[chips + 1 :]
    tok = q_refs[0].shape[0]
    total = chips * tok
    videos, half, text = tk_own.shape[1:]
    chip, core = my_chip(), my_core()
    for k in range(chips):
        qs[rows((chip ^ k) * tok, tok), :] = q_refs[k][...]
    qs[pl.ds(total, CHUNK), :] = jnp.zeros((CHUNK, HEAD_CHANNELS), qs.dtype)
    places = lax.broadcasted_iota(jnp.int32, (1, text), 1)
    start = jnp.int32(0)
    own_rows = pl.ds(pl.multiple_of(core * half, half), half)
    other_rows = pl.ds(pl.multiple_of((1 - core) * half, half), half)
    for video in range(videos):
        count = counts_ref[video]
        first = start
        tk[video, own_rows, :] = tk_own[core, video]
        tk[video, other_rows, :] = tk_other[core, video]
        tv[video, own_rows, :] = tv_own[core, video]
        tv[video, other_rows, :] = tv_other[core, video]
        live = places < lengths_ref[core, video]

        def chunk(index, carry):
            at = rows(first + index * CHUNK, CHUNK)
            scores = jnp.dot(qs[at, :], tk[video], preferred_element_type=jnp.float32)
            raised, sums = softmax_parts(jnp.where(live, scores, -1e30))
            out = lax.dot_general(
                raised.astype(jnp.bfloat16),
                tv[video],
                (((1,), (1,)), ((), ())),
                preferred_element_type=jnp.float32,
            )
            out_ref[at, :] = out / sums
            return carry

        length = count * TPF
        lax.fori_loop(0, (length + CHUNK - 1) // CHUNK, chunk, 0)
        start = start + length


def self_kernel(chips, counts_ref, cross_ref, *rest):
    q_refs, kv_refs = rest[:chips], rest[chips : 2 * chips]
    outs = rest[2 * chips : 3 * chips]
    ks, vs = rest[3 * chips : 3 * chips + 2]
    tok = q_refs[0].shape[0]
    total = chips * tok
    chip = my_chip()
    for k in range(chips):
        at = rows((chip ^ k) * tok, tok)
        ks[at, :] = kv_refs[k][pl.ds(0, tok), :]
        vs[at, :] = kv_refs[k][pl.ds(tok, tok), :]
    ends, end = [], jnp.int32(0)
    for video in range(counts_ref.shape[0]):
        end = end + counts_ref[video] * TPF
        ends.append(end)

    def video_of(place):
        return sum((place >= e).astype(jnp.int32) for e in ends[:-1])

    key_video = video_of(lax.broadcasted_iota(jnp.int32, (1, total), 1))

    def attend(queries, base):
        query_video = video_of(base + lax.broadcasted_iota(jnp.int32, (tok, 1), 0))
        scores = lax.dot_general(
            queries, ks[...], (((1,), (1,)), ((), ())), preferred_element_type=jnp.float32
        )
        raised, sums = softmax_parts(jnp.where(query_video == key_video, scores, -1e30))
        out = jnp.dot(raised.astype(jnp.bfloat16), vs[...], preferred_element_type=jnp.float32)
        return (out / sums + cross_ref[rows(base, tok), :]).astype(jnp.bfloat16)

    if chips <= UNROLL_CHIPS:
        for k in range(chips):
            outs[k][...] = attend(q_refs[k][...], (chip ^ k) * tok)
        return
    staged = rest[3 * chips + 2]
    for k in range(chips):
        staged[k] = q_refs[k][...]

    def block(k, carry):
        staged[k] = attend(staged[k], (chip ^ k) * tok)
        return carry

    lax.fori_loop(0, chips, block, 0)
    for k in range(chips):
        outs[k][...] = staged[k]


def head_kernel(chips, scale_ref, x_ref, gain_ref, shift_ref, weight_ref, bias_ref, *rest):
    blocks, keep_ref, send_ref, joined, moved = rest[:chips], *rest[chips:]
    tok = x_ref.shape[0]
    half = tok // 2
    chip, core = my_chip(), my_core()
    for k in range(chips):
        joined[chip ^ k] = blocks[k][...]
    width = x_ref.shape[1]
    attention = jnp.concatenate([joined[h] for h in range(chips)], axis=-1)
    hidden = x_ref[...].astype(jnp.float32) + attention.astype(jnp.float32)
    mean = jnp.sum(hidden, axis=-1, keepdims=True) * (1.0 / width)
    centred = hidden - mean
    var = jnp.sum(centred * centred, axis=-1, keepdims=True) * (1.0 / width)
    normed = centred * lax.rsqrt(var + 1e-06) * gain_ref[...] + shift_ref[...]
    velocity = lax.dot_general(
        normed.astype(jnp.bfloat16),
        weight_ref[...],
        (((1,), (1,)), ((), ())),
        preferred_element_type=jnp.float32,
    )
    scale = scale_ref[0]
    moved[...] = (velocity + bias_ref[...]) * jnp.where(core == 0, scale, 1.0 - scale)
    keep_ref[...] = moved[pl.ds(pl.multiple_of(core * half, 8), half), :]
    send_ref[...] = moved[pl.ds(pl.multiple_of((1 - core) * half, 8), half), :]


def local(
    queries,
    self_keys,
    self_values,
    residual_in,
    text_keys,
    text_values,
    text_lengths,
    frame_counts,
    mod_gain,
    mod_shift,
    head_weight,
    head_bias,
    guide_scale,
):
    devices = lax.axis_size("seq")
    chips = devices // 2
    tok, width = queries.shape
    total = chips * tok
    bf16, f32 = jnp.bfloat16, jnp.float32
    q_shape = jax.ShapeDtypeStruct((tok, HEAD_CHANNELS), bf16)
    kv_shape = jax.ShapeDtypeStruct((2 * tok, HEAD_CHANNELS), bf16)

    packed = pl.pallas_call(
        functools.partial(pack_kernel, chips),
        out_shape=[q_shape] * chips + [kv_shape] * chips,
        in_specs=[ANY] * 3,
        out_specs=[VMEM] * (2 * chips),
        scratch_shapes=[pltpu.SemaphoreType.DMA((3 * chips,))],
        name="pack",
    )(queries, self_keys, self_values)
    text_keys = jnp.swapaxes(text_keys, 2, 3)
    text_values = jnp.swapaxes(text_values, 2, 3)
    other_keys = lax.ppermute(text_keys, "seq", core_pairs(devices))
    other_values = lax.ppermute(text_values, "seq", core_pairs(devices))

    order = sorted(range(1, chips), reverse=True)
    q_blocks, kv_blocks = list(packed[:chips]), list(packed[chips:])
    for k in order:
        q_blocks[k] = lax.ppermute(q_blocks[k], "seq", chip_pairs(devices, k))
    for k in order:
        kv_blocks[k] = lax.ppermute(kv_blocks[k], "seq", chip_pairs(devices, k))

    videos, half, text = text_keys.shape[1:]
    cross = pl.pallas_call(
        functools.partial(cross_kernel, chips),
        out_shape=jax.ShapeDtypeStruct((total + CHUNK, HEAD_CHANNELS), f32),
        in_specs=[SMEM] * 2 + [VMEM] * (4 + chips),
        out_specs=VMEM,
        scratch_shapes=[
            pltpu.VMEM((total + CHUNK, HEAD_CHANNELS), bf16),
            pltpu.VMEM((videos, 2 * half, text), bf16),
            pltpu.VMEM((videos, 2 * half, text), bf16),
        ],
        cost_estimate=pl.CostEstimate(
            flops=8 * total * text * HEAD_CHANNELS,
            bytes_accessed=4 * total * HEAD_CHANNELS,
            transcendentals=total * text,
        ),
        name="cross",
    )(frame_counts, text_lengths, text_keys, text_values, other_keys, other_values, *q_blocks)

    staged = [] if chips <= UNROLL_CHIPS else [pltpu.VMEM((chips, tok, HEAD_CHANNELS), bf16)]
    blocks = pl.pallas_call(
        functools.partial(self_kernel, chips),
        out_shape=[q_shape] * chips,
        in_specs=[SMEM] + [VMEM] * (1 + 2 * chips),
        out_specs=[VMEM] * chips,
        scratch_shapes=[
            pltpu.VMEM((total, HEAD_CHANNELS), bf16),
            pltpu.VMEM((total, HEAD_CHANNELS), bf16),
        ]
        + staged,
        cost_estimate=pl.CostEstimate(
            flops=4 * total * total * HEAD_CHANNELS,
            bytes_accessed=8 * total * HEAD_CHANNELS,
            transcendentals=total * total,
        ),
        name="self",
    )(frame_counts, cross, *q_blocks, *kv_blocks)

    blocks = list(blocks)
    for k in order:
        blocks[k] = lax.ppermute(blocks[k], "seq", chip_pairs(devices, k))

    outs = head_weight.shape[1]
    part = jax.ShapeDtypeStruct((tok // 2, outs), f32)
    keep, send = pl.pallas_call(
        functools.partial(head_kernel, chips),
        out_shape=[part, part],
        in_specs=[SMEM] + [VMEM] * (5 + chips),
        out_specs=[VMEM] * 2,
        scratch_shapes=[
            pltpu.VMEM((chips, tok, HEAD_CHANNELS), bf16),
            pltpu.VMEM((tok, outs), f32),
        ],
        name="head",
    )(
        guide_scale,
        residual_in,
        mod_gain.reshape(1, width),
        mod_shift.reshape(1, width),
        head_weight.T,
        head_bias.reshape(1, outs),
        *blocks,
    )
    return keep + lax.ppermute(send, "seq", core_pairs(devices))


def solution(mesh):
    return jax.shard_map(
        local,
        mesh=mesh,
        in_specs=(
            P(("parts", "seq"), None),
            P(("parts", "seq"), None),
            P(("parts", "seq"), None),
            P(("parts", "seq"), None),
            P(None, "parts", None, "seq"),
            P(None, "parts", None, "seq"),
            P(None, "parts"),
            P("parts"),
            P(),
            P(),
            P(),
            P(),
            P(),
        ),
        out_specs=P(("parts", "seq"), None),
        check_vma=False,
    )
```

```python
import functools
import math

import jax
import jax.numpy as jnp
from jax import lax
from jax.experimental import pallas as pl
from jax.experimental.pallas import tpu as pltpu
from jax.sharding import PartitionSpec as P

HEAD_CHANNELS = 128
TPF = 32
SCALE = HEAD_CHANNELS ** (-0.5)
LOG2E = math.log2(math.e)
UNROLL_CHIPS = 8
STRIP = 8
LATE = 3


def params(mib):
    return pltpu.CompilerParams(vmem_limit_bytes=mib << 20)


VMEM = pl.BlockSpec(memory_space=pltpu.VMEM)
SMEM = pl.BlockSpec(memory_space=pltpu.SMEM)
HBM = pl.BlockSpec(memory_space=pltpu.HBM)


def chip_pairs(devices, index):
    return [(d, d ^ (2 * hop(index, devices // 2, d % 2))) for d in range(devices)]


def core_pairs(devices):
    return [(source, source ^ 1) for source in range(devices)]


def hop(index, chips, core):
    return (1 - core) * (index // 2 + (index % 2) * (chips // 2)) + core * (index)


def my_chip():
    return lax.axis_index("seq") // 2


def my_core():
    return lax.axis_index("seq") % 2


def rows(start, size):
    if isinstance(start, int):
        return pl.ds(start, size)
    return pl.ds(pl.multiple_of(start, TPF), size)


def pack_kernel(chips, *refs):
    sources, small, residual = refs[:3], refs[3:6], refs[6]
    blocks, kept, (own, other, sems) = refs[7 : 7 + chips], refs[7 + chips : 10 + chips], refs[10 + chips :]
    tok = sources[0].shape[0]
    chip, core = my_chip(), my_core()
    copies = []
    for index in range(chips):
        head = chip ^ hop(index, chips, core)
        cols = pl.ds(pl.multiple_of(head * HEAD_CHANNELS, HEAD_CHANNELS), HEAD_CHANNELS)
        for part, source in enumerate(sources):
            target = blocks[index].at[pl.ds(part * tok, tok)]
            copies.append(pltpu.make_async_copy(source.at[:, cols], target, sems.at[len(copies)]))
    half = tok // 2
    halves = [residual.at[pl.ds(pl.multiple_of(c * half, 16), half)] for c in (core, 1 - core)]
    for source, target in zip(list(small) + halves, list(kept) + [own, other]):
        copies.append(pltpu.make_async_copy(source, target, sems.at[len(copies)]))
    for copy in copies:
        copy.start()
    for copy in copies:
        copy.wait()


def softmax(scores):
    top = jnp.max(scores, axis=-1, keepdims=True)
    raised = jnp.exp2((scores - top) * (SCALE * LOG2E))
    share = 1.0 / jnp.sum(raised, axis=-1, keepdims=True)
    return (raised * share).astype(jnp.bfloat16)


def repeat(count, body):
    if count <= UNROLL_CHIPS:
        for index in range(count):
            body(index, 0)
    else:
        lax.fori_loop(0, count, body, 0)


def dot_last(a, b):
    return lax.dot_general(a, b, (((1,), (1,)), ((), ())), preferred_element_type=jnp.float32)


def video_ends(counts_ref):
    ends, end = [], jnp.int32(0)
    for video in range(counts_ref.shape[0]):
        end = end + counts_ref[video] * TPF
        ends.append(end)
    return ends


def video_of(place, ends):
    return sum((place >= e).astype(jnp.int32) for e in ends[:-1])


def prompt(queries, keys, values, length):
    scores = jnp.dot(queries, keys, preferred_element_type=jnp.float32)
    place = lax.broadcasted_iota(jnp.int32, (1, keys.shape[1]), 1)
    return dot_last(softmax(jnp.where(place < length, scores, -1e30)), values)


def early_kernel(chips, counts_ref, lengths_ref, tk_own, tv_own, tk_other, tv_other, *rest):
    blocks = rest[:-4]
    cross, tk, tv, qs = rest[-4:]
    early, tok = cross.shape[:2]
    videos, half = tk_own.shape[1:3]
    chip, core = my_chip(), my_core()
    ends = video_ends(counts_ref)
    own_rows = pl.ds(pl.multiple_of(core * half, half), half)
    other_rows = pl.ds(pl.multiple_of((1 - core) * half, half), half)
    for video in range(videos):
        tk[video, own_rows, :] = tk_own[core, video]
        tk[video, other_rows, :] = tk_other[core, video]
        tv[video, own_rows, :] = tv_own[core, video]
        tv[video, other_rows, :] = tv_other[core, video]
    for index in range(early):
        qs[index] = blocks[index][pl.ds(0, tok), :]

    def one(index, carry):
        video = video_of((chip ^ hop(index, chips, core)) * tok, ends)
        cross[index] = prompt(qs[index], tk[video], tv[video], lengths_ref[core, video])
        return carry

    repeat(early, one)


def attend_kernel(chips, counts_ref, lengths_ref, tk, tv, early_ref, *rest):
    blocks, out_ref = rest[:chips], rest[chips]
    qs, ks, vs, cross, raw, weights = rest[chips + 1 :]
    tok = cross.shape[1]
    total = chips * tok
    strip = raw.shape[0]
    chip, core = my_chip(), my_core()
    ends = video_ends(counts_ref)
    for index in range(chips):
        h = chip ^ hop(index, chips, core)
        at = rows(h * tok, tok)
        for part, target in enumerate((qs, ks, vs)):
            target[at, :] = blocks[index][pl.ds(part * tok, tok), :]

    def prompt_of(h, video):
        queries = qs[rows(h * tok, tok), :]
        return prompt(queries, tk[video], tv[video], lengths_ref[core, video])

    for index in range(chips):
        h = chip ^ hop(index, chips, core)
        if index < early_ref.shape[0]:
            cross[h] = early_ref[index]
        else:
            cross[h] = prompt_of(h, video_of(h * tok, ends))
    for video in range(1, len(ends)):
        h = ends[video - 1] // tok
        row_video = video_of(h * tok + lax.broadcasted_iota(jnp.int32, (tok, 1), 0), ends)
        cross[h] = jnp.where(row_video == video, prompt_of(h, video), cross[h])

    key_video = video_of(lax.broadcasted_iota(jnp.int32, (1, total), 1), ends)

    def one_strip(index, carry):
        base = index * strip
        raw[...] = dot_last(qs[rows(base, strip), :], ks[...])
        for b in range(strip // tok):
            at = pl.ds(b * tok, tok)
            place = base + b * tok + lax.broadcasted_iota(jnp.int32, (tok, 1), 0)
            allowed = video_of(place, ends) == key_video
            weights[at, :] = softmax(jnp.where(allowed, raw[at, :], -1e30))
        out = jnp.dot(weights[...], vs[...], preferred_element_type=jnp.float32)
        for b in range(strip // tok):
            h = index * (strip // tok) + b
            out_ref[h] = (out[b * tok : (b + 1) * tok] + cross[h]).astype(jnp.bfloat16)
        return carry

    repeat(total // strip, one_strip)


def head_kernel(chips, scale_ref, x_ref, x_other, gain_ref, shift_ref, weight_ref, bias_ref, blocks, out_ref):
    _, width = x_ref.shape
    core = my_core()
    gain, shift = (ref[...].reshape(1, width) for ref in (gain_ref, shift_ref))

    def velocity(x, branch):
        attention = jnp.concatenate([blocks[2 * h + branch] for h in range(chips)], axis=-1)
        hidden = x.astype(jnp.float32) + attention.astype(jnp.float32)
        mean = jnp.sum(hidden, axis=-1, keepdims=True) * (1.0 / width)
        centred = hidden - mean
        var = jnp.sum(centred * centred, axis=-1, keepdims=True) * (1.0 / width)
        normed = centred * lax.rsqrt(var + 1e-06) * gain + shift
        return dot_last(normed.astype(jnp.bfloat16), weight_ref[...]) + bias_ref[...].reshape(1, -1)

    own, other = velocity(x_ref[...], core), velocity(x_other[...], 1 - core)
    scale = scale_ref[0]
    share = jnp.where(core == 0, scale, 1.0 - scale)
    out_ref[...] = other + share * (own - other)


def local(
    queries,
    self_keys,
    self_values,
    residual_in,
    text_keys,
    text_values,
    text_lengths,
    frame_counts,
    mod_gain,
    mod_shift,
    head_weight,
    head_bias,
    guide_scale,
):
    devices = lax.axis_size("seq")
    chips = devices // 2
    tok, width = queries.shape
    total = chips * tok
    bf16, f32 = jnp.bfloat16, jnp.float32
    block_shape = jax.ShapeDtypeStruct((3 * tok, HEAD_CHANNELS), bf16)
    text_keys = jnp.swapaxes(text_keys, 2, 3)
    text_values = jnp.swapaxes(text_values, 2, 3)
    vectors = (mod_gain, mod_shift, head_bias)
    packed = pl.pallas_call(
        functools.partial(pack_kernel, chips),
        out_shape=[block_shape] * chips + [jax.ShapeDtypeStruct(v.shape, v.dtype) for v in vectors]
        + [jax.ShapeDtypeStruct((tok // 2, width), bf16)] * 2,
        in_specs=[HBM] * 7,
        out_specs=[VMEM] * (chips + 5),
        scratch_shapes=[pltpu.SemaphoreType.DMA((3 * chips + 5,))],
        compiler_params=params(8),
        name="pack",
    )(*(pltpu.with_memory_space_constraint(x, pltpu.HBM) for x in (queries, self_keys, self_values) + vectors + (residual_in,)))
    blocks, vectors, (x_own, x_other) = list(packed[:chips]), packed[chips:-2], packed[-2:]
    for index in range(1, chips):
        blocks[index] = lax.ppermute(blocks[index], "seq", chip_pairs(devices, index))
    other_keys = lax.ppermute(text_keys, "seq", core_pairs(devices))
    other_values = lax.ppermute(text_values, "seq", core_pairs(devices))
    x_other = lax.ppermute(x_other, "seq", core_pairs(devices))

    videos, half, text = text_keys.shape[1:]
    tokens = pltpu.VMEM((total, HEAD_CHANNELS), bf16)
    strip = math.gcd(chips, STRIP) * tok
    early = max(chips - LATE, 1)
    prompts = jax.ShapeDtypeStruct((videos, 2 * half, text), bf16)
    cross, keys, values = pl.pallas_call(
        functools.partial(early_kernel, chips),
        out_shape=[
            jax.ShapeDtypeStruct((early, tok, HEAD_CHANNELS), f32),
            prompts,
            prompts,
        ],
        in_specs=[SMEM] * 2 + [VMEM] * (4 + early),
        out_specs=[VMEM] * 3,
        scratch_shapes=[pltpu.VMEM((early, tok, HEAD_CHANNELS), bf16)],
        cost_estimate=pl.CostEstimate(
            flops=4 * early * tok * text * HEAD_CHANNELS,
            bytes_accessed=4 * total * HEAD_CHANNELS,
            transcendentals=early * tok * text,
        ),
        compiler_params=params(12),
        name="early",
    )(frame_counts, text_lengths, text_keys, text_values, other_keys, other_values, *blocks[:early])
    attended = pl.pallas_call(
        functools.partial(attend_kernel, chips),
        out_shape=jax.ShapeDtypeStruct((chips, tok, HEAD_CHANNELS), bf16),
        in_specs=[SMEM] * 2 + [VMEM] * (3 + chips),
        out_specs=VMEM,
        scratch_shapes=[tokens] * 3
        + [
            pltpu.VMEM((chips, tok, HEAD_CHANNELS), f32),
            pltpu.VMEM((strip, total), f32),
            pltpu.VMEM((strip, total), bf16),
        ],
        cost_estimate=pl.CostEstimate(
            flops=4 * total * total * HEAD_CHANNELS,
            bytes_accessed=8 * total * HEAD_CHANNELS,
            transcendentals=total * total,
        ),
        compiler_params=params(24),
        name="attend",
    )(frame_counts, text_lengths, keys, values, cross, *blocks)
    returned = lax.all_to_all(
        attended.reshape(devices, tok // 2, HEAD_CHANNELS), "seq", split_axis=0, concat_axis=0, tiled=True
    )

    return pl.pallas_call(
        functools.partial(head_kernel, chips),
        out_shape=jax.ShapeDtypeStruct((tok // 2, head_weight.shape[1]), f32),
        in_specs=[SMEM] + [VMEM] * 7,
        out_specs=VMEM,
        compiler_params=params(8),
        name="head",
    )(guide_scale, x_own, x_other, vectors[0], vectors[1], head_weight.T, vectors[2], returned)


def solution(mesh):
    return jax.shard_map(
        local,
        mesh=mesh,
        in_specs=(
            P(("parts", "seq"), None),
            P(("parts", "seq"), None),
            P(("parts", "seq"), None),
            P(("parts", "seq"), None),
            P(None, "parts", None, "seq"),
            P(None, "parts", None, "seq"),
            P(None, "parts"),
            P("parts"),
            P(),
            P(),
            P(),
            P(),
            P(),
        ),
        out_specs=P(("parts", "seq"), None),
        check_vma=False,
    )
```

```python
import functools
import math

import jax
import jax.numpy as jnp
from jax import lax
from jax.experimental import pallas as pl
from jax.experimental.pallas import tpu as pltpu
from jax.sharding import PartitionSpec as P

HEAD_CHANNELS = 128
TPF = 32
SCALE = HEAD_CHANNELS ** (-0.5)
LOG2E = math.log2(math.e)
UNROLL_CHIPS = 8
STRIP = 8
LATE = 3


def params(mib):
    return pltpu.CompilerParams(vmem_limit_bytes=mib << 20)


VMEM = pl.BlockSpec(memory_space=pltpu.VMEM)
SMEM = pl.BlockSpec(memory_space=pltpu.SMEM)
HBM = pl.BlockSpec(memory_space=pltpu.HBM)


def chip_pairs(devices, index):
    return [(d, d ^ (2 * hop(index, devices // 2))) for d in range(devices)]


def core_pairs(devices):
    return [(source, source ^ 1) for source in range(devices)]


def hop(index, chips):
    near = index // 2
    return near + (index % 2) * (chips - 1 - 2 * near)


def my_chip():
    return lax.axis_index("seq") // 2


def my_core():
    return lax.axis_index("seq") % 2


def rows(start, size):
    if isinstance(start, int):
        return pl.ds(start, size)
    return pl.ds(pl.multiple_of(start, TPF), size)


def pack_kernel(chips, *refs):
    sources, blocks, sems = refs[:3], refs[3 : 3 + chips], refs[3 + chips]
    tok = sources[0].shape[0]
    chip = my_chip()
    copies = []
    for index in range(chips):
        head = chip ^ hop(index, chips)
        cols = pl.ds(pl.multiple_of(head * HEAD_CHANNELS, HEAD_CHANNELS), HEAD_CHANNELS)
        for part, source in enumerate(sources):
            target = blocks[index].at[pl.ds(part * tok, tok)]
            copies.append(pltpu.make_async_copy(source.at[:, cols], target, sems.at[len(copies)]))
    for copy in copies:
        copy.start()
    for copy in copies:
        copy.wait()


def softmax(scores):
    top = jnp.max(scores, axis=-1, keepdims=True)
    raised = jnp.exp2((scores - top) * (SCALE * LOG2E))
    share = 1.0 / jnp.sum(raised, axis=-1, keepdims=True)
    return (raised * share).astype(jnp.bfloat16)


def repeat(count, body):
    if count <= UNROLL_CHIPS:
        for index in range(count):
            body(index, 0)
    else:
        lax.fori_loop(0, count, body, 0)


def dot_last(a, b):
    return lax.dot_general(a, b, (((1,), (1,)), ((), ())), preferred_element_type=jnp.float32)


def video_ends(counts_ref):
    ends, end = [], jnp.int32(0)
    for video in range(counts_ref.shape[0]):
        end = end + counts_ref[video] * TPF
        ends.append(end)
    return ends


def video_of(place, ends):
    place = jnp.int32(place) if isinstance(place, int) else place
    return sum((place >= e).astype(jnp.int32) for e in ends[:-1])


def prompts(picked, raw, shares):
    tok, text = picked[0][0].shape[0], raw.shape[1]
    place = lax.broadcasted_iota(jnp.int32, (1, text), 1)
    for i, (queries, keys, _, _) in enumerate(picked):
        raw[pl.ds(i * tok, tok), :] = jnp.dot(queries, keys, preferred_element_type=jnp.float32)
    for i, (_, _, _, length) in enumerate(picked):
        for frame in range(tok // TPF):
            at = pl.ds(i * tok + frame * TPF, TPF)
            shares[at, :] = softmax(jnp.where(place < length, raw[at, :], -1e30))
    return [dot_last(shares[pl.ds(i * tok, tok), :], p[2]) for i, p in enumerate(picked)]


def early_kernel(chips, counts_ref, lengths_ref, tk_own, tv_own, tk_other, tv_other, *rest):
    early, tok = rest[-11].shape[:2]
    small, residual, blocks = rest[:3], rest[3], rest[4 : 4 + early]
    cross, tk, tv, *kept, own, other, raw, shares, sems = rest[4 + early :]
    videos, half = tk_own.shape[1:3]
    chip, core = my_chip(), my_core()
    sides = [residual.at[pl.ds(pl.multiple_of(c * (tok // 2), 16), tok // 2)] for c in (core, 1 - core)]
    copies = [
        pltpu.make_async_copy(source, target, sems.at[i])
        for i, (source, target) in enumerate(zip((*small, *sides), (*kept, own, other)))
    ]
    for copy in copies:
        copy.start()
    ends = video_ends(counts_ref)
    own_rows = pl.ds(pl.multiple_of(core * half, half), half)
    other_rows = pl.ds(pl.multiple_of((1 - core) * half, half), half)
    for video in range(videos):
        tk[video, own_rows, :] = tk_own[core, video]
        tk[video, other_rows, :] = tk_other[core, video]
        tv[video, own_rows, :] = tv_own[core, video]
        tv[video, other_rows, :] = tv_other[core, video]
    picked = []
    for index in range(early):
        video = video_of((chip ^ hop(index, chips)) * tok, ends)
        queries = blocks[index][pl.ds(0, tok), :]
        picked.append((queries, tk[video], tv[video], lengths_ref[core, video]))
    for index, out in enumerate(prompts(picked, raw, shares)):
        cross[index] = out
    for copy in copies:
        copy.wait()


def attend_kernel(chips, counts_ref, lengths_ref, tk, tv, early_ref, *rest):
    blocks, out_ref = rest[:chips], rest[chips]
    qs, ks, vs, cross, raw, weights, prompt_raw, shares = rest[chips + 1 :]
    tok = cross.shape[1]
    total = chips * tok
    strip = raw.shape[0]
    chip, core = my_chip(), my_core()
    ends = video_ends(counts_ref)
    for index in range(chips):
        h = chip ^ hop(index, chips)
        at = rows(h * tok, tok)
        for part, target in enumerate((qs, ks, vs)):
            target[at, :] = blocks[index][pl.ds(part * tok, tok), :]

    def pick(h, video):
        queries = qs[rows(h * tok, tok), :]
        return queries, tk[video], tv[video], lengths_ref[core, video]

    early = early_ref.shape[0]
    late = [chip ^ hop(index, chips) for index in range(early, chips)]
    begun = [ends[video - 1] // tok for video in range(1, len(ends))]
    picked = [pick(h, video_of(h * tok, ends)) for h in late]
    picked += [pick(h, video + 1) for video, h in enumerate(begun)]
    found = prompts(picked, prompt_raw, shares)
    for index in range(early):
        cross[chip ^ hop(index, chips)] = early_ref[index]
    for h, out in zip(late, found):
        cross[h] = out
    for video, (h, out) in enumerate(zip(begun, found[len(late) :])):
        for frame in range(tok // TPF):
            at = pl.ds(frame * TPF, TPF)
            here = video_of(h * tok + frame * TPF, ends) == video + 1
            cross[h, at, :] = jnp.where(here, out[frame * TPF : (frame + 1) * TPF], cross[h, at, :])

    key_video = video_of(lax.broadcasted_iota(jnp.int32, (1, total), 1), ends)

    def one_strip(index, carry):
        base = index * strip
        raw[...] = dot_last(qs[rows(base, strip), :], ks[...])
        for frame in range(strip // TPF):
            at = pl.ds(frame * TPF, TPF)
            allowed = key_video == video_of(base + frame * TPF, ends)
            weights[at, :] = softmax(jnp.where(allowed, raw[at, :], -1e30))
        out = jnp.dot(weights[...], vs[...], preferred_element_type=jnp.float32)
        for b in range(strip // tok):
            h = index * (strip // tok) + b
            out_ref[h] = (out[b * tok : (b + 1) * tok] + cross[h]).astype(jnp.bfloat16)
        return carry

    repeat(total // strip, one_strip)


def head_kernel(chips, scale_ref, x_ref, x_other, gain_ref, shift_ref, weight_ref, bias_ref, blocks, out_ref):
    _, width = x_ref.shape
    core = my_core()
    gain, shift = (ref[...].reshape(1, width) for ref in (gain_ref, shift_ref))

    def velocity(x, branch):
        attention = jnp.concatenate([blocks[2 * h + branch] for h in range(chips)], axis=-1)
        hidden = x.astype(jnp.float32) + attention.astype(jnp.float32)
        mean = jnp.sum(hidden, axis=-1, keepdims=True) * (1.0 / width)
        centred = hidden - mean
        var = jnp.sum(centred * centred, axis=-1, keepdims=True) * (1.0 / width)
        normed = centred * lax.rsqrt(var + 1e-06) * gain + shift
        return dot_last(normed.astype(jnp.bfloat16), weight_ref[...]) + bias_ref[...].reshape(1, -1)

    own, other = velocity(x_ref[...], core), velocity(x_other[...], 1 - core)
    scale = scale_ref[0]
    share = jnp.where(core == 0, scale, 1.0 - scale)
    out_ref[...] = other + share * (own - other)


def local(
    queries,
    self_keys,
    self_values,
    residual_in,
    text_keys,
    text_values,
    text_lengths,
    frame_counts,
    mod_gain,
    mod_shift,
    head_weight,
    head_bias,
    guide_scale,
):
    devices = lax.axis_size("seq")
    chips = devices // 2
    tok, width = queries.shape
    total = chips * tok
    bf16, f32 = jnp.bfloat16, jnp.float32
    block_shape = jax.ShapeDtypeStruct((3 * tok, HEAD_CHANNELS), bf16)
    text_keys = jnp.swapaxes(text_keys, 2, 3)
    text_values = jnp.swapaxes(text_values, 2, 3)
    vectors = (mod_gain, mod_shift, head_bias)
    packed = pl.pallas_call(
        functools.partial(pack_kernel, chips),
        out_shape=[block_shape] * chips,
        in_specs=[HBM] * 3,
        out_specs=[VMEM] * chips,
        scratch_shapes=[pltpu.SemaphoreType.DMA((3 * chips,))],
        compiler_params=params(8),
        name="pack",
    )(*(pltpu.with_memory_space_constraint(x, pltpu.HBM) for x in (queries, self_keys, self_values)))
    blocks = list(packed)
    for index in range(1, chips):
        blocks[index] = lax.ppermute(blocks[index], "seq", chip_pairs(devices, index))
    other_keys = lax.ppermute(text_keys, "seq", core_pairs(devices))
    other_values = lax.ppermute(text_values, "seq", core_pairs(devices))
    videos, half, text = text_keys.shape[1:]
    tokens = pltpu.VMEM((total, HEAD_CHANNELS), bf16)
    strip = math.gcd(chips, STRIP) * tok
    early = max(chips - LATE, 1)
    joined = jax.ShapeDtypeStruct((videos, 2 * half, text), bf16)
    cross, keys, values, *vectors, x_own, x_other = pl.pallas_call(
        functools.partial(early_kernel, chips),
        out_shape=[
            jax.ShapeDtypeStruct((early, tok, HEAD_CHANNELS), f32),
            joined,
            joined,
        ]
        + [jax.ShapeDtypeStruct(v.shape, v.dtype) for v in vectors]
        + [jax.ShapeDtypeStruct((tok // 2, width), bf16)] * 2,
        in_specs=[SMEM] * 2 + [VMEM] * 4 + [HBM] * 4 + [VMEM] * early,
        out_specs=[VMEM] * 8,
        scratch_shapes=[
            pltpu.VMEM((early * tok, text), f32),
            pltpu.VMEM((early * tok, text), bf16),
            pltpu.SemaphoreType.DMA((5,)),
        ],
        cost_estimate=pl.CostEstimate(
            flops=4 * early * tok * text * HEAD_CHANNELS,
            bytes_accessed=4 * total * HEAD_CHANNELS,
            transcendentals=early * tok * text,
        ),
        compiler_params=params(12),
        name="early",
    )(
        frame_counts,
        text_lengths,
        text_keys,
        text_values,
        other_keys,
        other_values,
        *(pltpu.with_memory_space_constraint(x, pltpu.HBM) for x in (*vectors, residual_in)),
        *blocks[:early],
    )
    x_other = lax.ppermute(x_other, "seq", core_pairs(devices))
    attended = pl.pallas_call(
        functools.partial(attend_kernel, chips),
        out_shape=jax.ShapeDtypeStruct((chips, tok, HEAD_CHANNELS), bf16),
        in_specs=[SMEM] * 2 + [VMEM] * (3 + chips),
        out_specs=VMEM,
        scratch_shapes=[tokens] * 3
        + [
            pltpu.VMEM((chips, tok, HEAD_CHANNELS), f32),
            pltpu.VMEM((strip, total), f32),
            pltpu.VMEM((strip, total), bf16),
            pltpu.VMEM(((chips - early + videos - 1) * tok, text), f32),
            pltpu.VMEM(((chips - early + videos - 1) * tok, text), bf16),
        ],
        cost_estimate=pl.CostEstimate(
            flops=4 * total * total * HEAD_CHANNELS,
            bytes_accessed=8 * total * HEAD_CHANNELS,
            transcendentals=total * total,
        ),
        compiler_params=params(24),
        name="attend",
    )(frame_counts, text_lengths, keys, values, cross, *blocks)
    returned = lax.all_to_all(
        attended.reshape(devices, tok // 2, HEAD_CHANNELS), "seq", split_axis=0, concat_axis=0, tiled=True
    )

    return pl.pallas_call(
        functools.partial(head_kernel, chips),
        out_shape=jax.ShapeDtypeStruct((tok // 2, head_weight.shape[1]), f32),
        in_specs=[SMEM] + [VMEM] * 7,
        out_specs=VMEM,
        compiler_params=params(8),
        name="head",
    )(guide_scale, x_own, x_other, vectors[0], vectors[1], head_weight.T, vectors[2], returned)


def solution(mesh):
    return jax.shard_map(
        local,
        mesh=mesh,
        in_specs=(
            P(("parts", "seq"), None),
            P(("parts", "seq"), None),
            P(("parts", "seq"), None),
            P(("parts", "seq"), None),
            P(None, "parts", None, "seq"),
            P(None, "parts", None, "seq"),
            P(None, "parts"),
            P("parts"),
            P(),
            P(),
            P(),
            P(),
            P(),
        ),
        out_specs=P(("parts", "seq"), None),
        check_vma=False,
    )
```

```python
import functools
import math

import jax
import jax.numpy as jnp
from jax import lax
from jax.experimental import pallas as pl
from jax.experimental.pallas import tpu as pltpu
from jax.sharding import PartitionSpec as P

HEAD_CHANNELS = 128
TPF = 32
SCALE = HEAD_CHANNELS ** (-0.5)
LOG2E = math.log2(math.e)
UNROLL_CHIPS = 8
STRIP = 8
LATE = 3
LEAD = 4


def params(mib):
    return pltpu.CompilerParams(vmem_limit_bytes=mib << 20)


VMEM = pl.BlockSpec(memory_space=pltpu.VMEM)
SMEM = pl.BlockSpec(memory_space=pltpu.SMEM)
HBM = pl.BlockSpec(memory_space=pltpu.HBM)


def chip_pairs(devices, index):
    return [(d, d ^ (2 * hop(index, devices // 2))) for d in range(devices)]


def core_pairs(devices):
    return [(source, source ^ 1) for source in range(devices)]


def hop(index, chips):
    near = index // 2
    return near + (index % 2) * (chips - 1 - 2 * near)


def lead(chips):
    return chips * LEAD // 8


def place_of(chip, chips):
    return (chip + chips - lead(chips)) % chips


def my_chip():
    return lax.axis_index("seq") // 2


def my_core():
    return lax.axis_index("seq") % 2


def rows(start, size):
    if isinstance(start, int):
        return pl.ds(start, size)
    return pl.ds(pl.multiple_of(start, TPF), size)


def pack_kernel(chips, *refs):
    sources, blocks, sems = refs[:3], refs[3 : 3 + chips], refs[3 + chips]
    tok = sources[0].shape[0]
    chip = my_chip()
    copies = []
    for index in range(chips):
        head = chip ^ hop(index, chips)
        cols = pl.ds(pl.multiple_of(head * HEAD_CHANNELS, HEAD_CHANNELS), HEAD_CHANNELS)
        for part, source in enumerate(sources):
            target = blocks[index].at[pl.ds(part * tok, tok)]
            copies.append(pltpu.make_async_copy(source.at[:, cols], target, sems.at[len(copies)]))
    for copy in copies:
        copy.start()
    for copy in copies:
        copy.wait()


def softmax(scores):
    top = jnp.max(scores, axis=-1, keepdims=True)
    raised = jnp.exp2((scores - top) * (SCALE * LOG2E))
    share = 1.0 / jnp.sum(raised, axis=-1, keepdims=True)
    return (raised * share).astype(jnp.bfloat16)


def repeat(count, body):
    if count <= UNROLL_CHIPS:
        for index in range(count):
            body(index, 0)
    else:
        lax.fori_loop(0, count, body, 0)


def dot_last(a, b):
    return lax.dot_general(a, b, (((1,), (1,)), ((), ())), preferred_element_type=jnp.float32)


def video_ends(counts_ref):
    ends, end = [], jnp.int32(0)
    for video in range(counts_ref.shape[0]):
        end = end + counts_ref[video] * TPF
        ends.append(end)
    return ends


def video_of(place, ends):
    place = jnp.int32(place) if isinstance(place, int) else place
    return sum((place >= e).astype(jnp.int32) for e in ends[:-1])


def prompts(picked, raw, shares):
    tok, text = picked[0][0].shape[0], raw.shape[1]
    place = lax.broadcasted_iota(jnp.int32, (1, text), 1)
    for i, (queries, keys, _, _) in enumerate(picked):
        raw[pl.ds(i * tok, tok), :] = jnp.dot(queries, keys, preferred_element_type=jnp.float32)
    for i, (_, _, _, length) in enumerate(picked):
        for frame in range(tok // TPF):
            at = pl.ds(i * tok + frame * TPF, TPF)
            shares[at, :] = softmax(jnp.where(place < length, raw[at, :], -1e30))
    return [dot_last(shares[pl.ds(i * tok, tok), :], p[2]) for i, p in enumerate(picked)]


def early_kernel(chips, counts_ref, lengths_ref, tk_own, tv_own, tk_other, tv_other, *rest):
    early, tok = rest[-11].shape[:2]
    small, residual, blocks = rest[:3], rest[3], rest[4 : 4 + early]
    cross, tk, tv, *kept, own, other, raw, shares, sems = rest[4 + early :]
    videos, half = tk_own.shape[1:3]
    chip, core = my_chip(), my_core()
    sides = [residual.at[pl.ds(pl.multiple_of(c * (tok // 2), 16), tok // 2)] for c in (core, 1 - core)]
    copies = [
        pltpu.make_async_copy(source, target, sems.at[i])
        for i, (source, target) in enumerate(zip((*small, *sides), (*kept, own, other)))
    ]
    for copy in copies:
        copy.start()
    ends = video_ends(counts_ref)
    own_rows = pl.ds(pl.multiple_of(core * half, half), half)
    other_rows = pl.ds(pl.multiple_of((1 - core) * half, half), half)
    for video in range(videos):
        tk[video, own_rows, :] = tk_own[core, video]
        tk[video, other_rows, :] = tk_other[core, video]
        tv[video, own_rows, :] = tv_own[core, video]
        tv[video, other_rows, :] = tv_other[core, video]
    picked = []
    for index in range(early):
        video = video_of((chip ^ hop(index, chips)) * tok, ends)
        queries = blocks[index][pl.ds(0, tok), :]
        picked.append((queries, tk[video], tv[video], lengths_ref[core, video]))
    for index, out in enumerate(prompts(picked, raw, shares)):
        cross[index] = out
    for copy in copies:
        copy.wait()


def attend_kernel(chips, counts_ref, lengths_ref, tk, tv, early_ref, *rest):
    blocks, out_ref = rest[:chips], rest[chips]
    qs, ks, vs, cross, raw, weights, prompt_raw, shares = rest[chips + 1 :]
    tok = cross.shape[1]
    total = chips * tok
    strip = raw.shape[0]
    chip, core = my_chip(), my_core()
    ends = video_ends(counts_ref)
    for index in range(chips):
        h = chip ^ hop(index, chips)
        at = rows(h * tok, tok)
        for part, target in enumerate((qs, ks, vs)):
            target[at, :] = blocks[index][pl.ds(part * tok, tok), :]

    def pick(h, video):
        queries = qs[rows(h * tok, tok), :]
        return queries, tk[video], tv[video], lengths_ref[core, video]

    early = early_ref.shape[0]
    late = [chip ^ hop(index, chips) for index in range(early, chips)]
    begun = [ends[video - 1] // tok for video in range(1, len(ends))]
    picked = [pick(h, video_of(h * tok, ends)) for h in late]
    picked += [pick(h, video + 1) for video, h in enumerate(begun)]
    found = prompts(picked, prompt_raw, shares)
    for index in range(early):
        cross[chip ^ hop(index, chips)] = early_ref[index]
    for h, out in zip(late, found):
        cross[h] = out
    for video, (h, out) in enumerate(zip(begun, found[len(late) :])):
        for frame in range(tok // TPF):
            at = pl.ds(frame * TPF, TPF)
            here = video_of(h * tok + frame * TPF, ends) == video + 1
            cross[h, at, :] = jnp.where(here, out[frame * TPF : (frame + 1) * TPF], cross[h, at, :])

    key_video = video_of(lax.broadcasted_iota(jnp.int32, (1, total), 1), ends)

    def one_strip(index, carry):
        base = index * strip
        raw[...] = dot_last(qs[rows(base, strip), :], ks[...])
        for frame in range(strip // TPF):
            at = pl.ds(frame * TPF, TPF)
            allowed = key_video == video_of(base + frame * TPF, ends)
            weights[at, :] = softmax(jnp.where(allowed, raw[at, :], -1e30))
        out = jnp.dot(weights[...], vs[...], preferred_element_type=jnp.float32)
        for b in range(strip // tok):
            h = index * (strip // tok) + b
            out_ref[place_of(h, chips)] = (out[b * tok : (b + 1) * tok] + cross[h]).astype(jnp.bfloat16)
        return carry

    repeat(total // strip, one_strip)


def head_kernel(chips, scale_ref, x_ref, x_other, gain_ref, shift_ref, weight_ref, bias_ref, blocks, out_ref):
    _, width = x_ref.shape
    core = my_core()
    gain, shift = (ref[...].reshape(1, width) for ref in (gain_ref, shift_ref))

    def velocity(x, branch):
        attention = jnp.concatenate([blocks[2 * place_of(h, chips) + branch] for h in range(chips)], axis=-1)
        hidden = x.astype(jnp.float32) + attention.astype(jnp.float32)
        mean = jnp.sum(hidden, axis=-1, keepdims=True) * (1.0 / width)
        centred = hidden - mean
        var = jnp.sum(centred * centred, axis=-1, keepdims=True) * (1.0 / width)
        normed = centred * lax.rsqrt(var + 1e-06) * gain + shift
        return dot_last(normed.astype(jnp.bfloat16), weight_ref[...]) + bias_ref[...].reshape(1, -1)

    own, other = velocity(x_ref[...], core), velocity(x_other[...], 1 - core)
    scale = scale_ref[0]
    share = jnp.where(core == 0, scale, 1.0 - scale)
    out_ref[...] = other + share * (own - other)


def local(
    queries,
    self_keys,
    self_values,
    residual_in,
    text_keys,
    text_values,
    text_lengths,
    frame_counts,
    mod_gain,
    mod_shift,
    head_weight,
    head_bias,
    guide_scale,
):
    devices = lax.axis_size("seq")
    chips = devices // 2
    tok, width = queries.shape
    total = chips * tok
    bf16, f32 = jnp.bfloat16, jnp.float32
    block_shape = jax.ShapeDtypeStruct((3 * tok, HEAD_CHANNELS), bf16)
    text_keys = jnp.swapaxes(text_keys, 2, 3)
    text_values = jnp.swapaxes(text_values, 2, 3)
    vectors = (mod_gain, mod_shift, head_bias)
    packed = pl.pallas_call(
        functools.partial(pack_kernel, chips),
        out_shape=[block_shape] * chips,
        in_specs=[HBM] * 3,
        out_specs=[VMEM] * chips,
        scratch_shapes=[pltpu.SemaphoreType.DMA((3 * chips,))],
        compiler_params=params(8),
        name="pack",
    )(*(pltpu.with_memory_space_constraint(x, pltpu.HBM) for x in (queries, self_keys, self_values)))
    blocks = list(packed)
    for index in range(1, chips):
        blocks[index] = lax.ppermute(blocks[index], "seq", chip_pairs(devices, index))
    other_keys = lax.ppermute(text_keys, "seq", core_pairs(devices))
    other_values = lax.ppermute(text_values, "seq", core_pairs(devices))
    videos, half, text = text_keys.shape[1:]
    tokens = pltpu.VMEM((total, HEAD_CHANNELS), bf16)
    strip = math.gcd(chips, STRIP) * tok
    early = max(chips - LATE, 1)
    joined = jax.ShapeDtypeStruct((videos, 2 * half, text), bf16)
    cross, keys, values, *vectors, x_own, x_other = pl.pallas_call(
        functools.partial(early_kernel, chips),
        out_shape=[
            jax.ShapeDtypeStruct((early, tok, HEAD_CHANNELS), f32),
            joined,
            joined,
        ]
        + [jax.ShapeDtypeStruct(v.shape, v.dtype) for v in vectors]
        + [jax.ShapeDtypeStruct((tok // 2, width), bf16)] * 2,
        in_specs=[SMEM] * 2 + [VMEM] * 4 + [HBM] * 4 + [VMEM] * early,
        out_specs=[VMEM] * 8,
        scratch_shapes=[
            pltpu.VMEM((early * tok, text), f32),
            pltpu.VMEM((early * tok, text), bf16),
            pltpu.SemaphoreType.DMA((5,)),
        ],
        cost_estimate=pl.CostEstimate(
            flops=4 * early * tok * text * HEAD_CHANNELS,
            bytes_accessed=4 * total * HEAD_CHANNELS,
            transcendentals=early * tok * text,
        ),
        compiler_params=params(12),
        name="early",
    )(
        frame_counts,
        text_lengths,
        text_keys,
        text_values,
        other_keys,
        other_values,
        *(pltpu.with_memory_space_constraint(x, pltpu.HBM) for x in (*vectors, residual_in)),
        *blocks[:early],
    )
    x_other = lax.ppermute(x_other, "seq", core_pairs(devices))
    attended = pl.pallas_call(
        functools.partial(attend_kernel, chips),
        out_shape=jax.ShapeDtypeStruct((chips, tok, HEAD_CHANNELS), bf16),
        in_specs=[SMEM] * 2 + [VMEM] * (3 + chips),
        out_specs=VMEM,
        scratch_shapes=[tokens] * 3
        + [
            pltpu.VMEM((chips, tok, HEAD_CHANNELS), f32),
            pltpu.VMEM((strip, total), f32),
            pltpu.VMEM((strip, total), bf16),
            pltpu.VMEM(((chips - early + videos - 1) * tok, text), f32),
            pltpu.VMEM(((chips - early + videos - 1) * tok, text), bf16),
        ],
        cost_estimate=pl.CostEstimate(
            flops=4 * total * total * HEAD_CHANNELS,
            bytes_accessed=8 * total * HEAD_CHANNELS,
            transcendentals=total * total,
        ),
        compiler_params=params(24),
        name="attend",
    )(frame_counts, text_lengths, keys, values, cross, *blocks)
    returned = lax.all_to_all(
        attended.reshape(devices, tok // 2, HEAD_CHANNELS),
        "seq",
        split_axis=0,
        concat_axis=0,
        axis_index_groups=[[(d + 2 * lead(chips)) % devices for d in range(devices)]],
        tiled=True,
    )

    return pl.pallas_call(
        functools.partial(head_kernel, chips),
        out_shape=jax.ShapeDtypeStruct((tok // 2, head_weight.shape[1]), f32),
        in_specs=[SMEM] + [VMEM] * 7,
        out_specs=VMEM,
        compiler_params=params(8),
        name="head",
    )(guide_scale, x_own, x_other, vectors[0], vectors[1], head_weight.T, vectors[2], returned)


def solution(mesh):
    return jax.shard_map(
        local,
        mesh=mesh,
        in_specs=(
            P(("parts", "seq"), None),
            P(("parts", "seq"), None),
            P(("parts", "seq"), None),
            P(("parts", "seq"), None),
            P(None, "parts", None, "seq"),
            P(None, "parts", None, "seq"),
            P(None, "parts"),
            P("parts"),
            P(),
            P(),
            P(),
            P(),
            P(),
        ),
        out_specs=P(("parts", "seq"), None),
        check_vma=False,
    )
```

```python
import functools
import math

import jax
import jax.numpy as jnp
from jax import lax
from jax.experimental import pallas as pl
from jax.experimental.pallas import tpu as pltpu
from jax.sharding import PartitionSpec as P

HEAD_CHANNELS = 128
TPF = 32
SCALE = HEAD_CHANNELS ** (-0.5)
LOG2E = math.log2(math.e)
UNROLL_CHIPS = 8
STRIP = 8
LATE = 3
LEAD = 4


def params(mib):
    return pltpu.CompilerParams(vmem_limit_bytes=mib << 20)


VMEM = pl.BlockSpec(memory_space=pltpu.VMEM)
SMEM = pl.BlockSpec(memory_space=pltpu.SMEM)
HBM = pl.BlockSpec(memory_space=pltpu.HBM)


def chip_pairs(devices, index):
    return [(d, d ^ (2 * hop(index, devices // 2))) for d in range(devices)]


def core_pairs(devices):
    return [(source, source ^ 1) for source in range(devices)]


def hop(index, chips):
    near = index // 2
    return near + (index % 2) * (chips - 1 - 2 * near)


def lead(chips):
    return chips * LEAD // 8


def place_of(chip, chips):
    return (chip + chips - lead(chips)) % chips


def my_chip():
    return lax.axis_index("seq") // 2


def my_core():
    return lax.axis_index("seq") % 2


def rows(start, size):
    if isinstance(start, int):
        return pl.ds(start, size)
    return pl.ds(pl.multiple_of(start, TPF), size)


def pack_kernel(chips, *refs):
    sources, blocks, sems = refs[:3], refs[3 : 3 + chips], refs[3 + chips]
    tok = sources[0].shape[0]
    chip = my_chip()
    copies = []
    for index in range(chips):
        head = chip ^ hop(index, chips)
        cols = pl.ds(pl.multiple_of(head * HEAD_CHANNELS, HEAD_CHANNELS), HEAD_CHANNELS)
        for part, source in enumerate(sources):
            target = blocks[index].at[pl.ds(part * tok, tok)]
            copies.append(pltpu.make_async_copy(source.at[:, cols], target, sems.at[len(copies)]))
    for copy in copies:
        copy.start()
    for copy in copies:
        copy.wait()


def softmax(scores):
    top = jnp.max(scores, axis=-1, keepdims=True)
    raised = jnp.exp2((scores - top) * (SCALE * LOG2E))
    share = 1.0 / jnp.sum(raised, axis=-1, keepdims=True)
    return (raised * share).astype(jnp.bfloat16)


def repeat(count, body):
    if count <= UNROLL_CHIPS:
        for index in range(count):
            body(index, 0)
    else:
        lax.fori_loop(0, count, body, 0)


def dot_last(a, b):
    return lax.dot_general(a, b, (((1,), (1,)), ((), ())), preferred_element_type=jnp.float32)


def video_ends(counts_ref):
    ends, end = [], jnp.int32(0)
    for video in range(counts_ref.shape[0]):
        end = end + counts_ref[video] * TPF
        ends.append(end)
    return ends


def video_of(place, ends):
    place = jnp.int32(place) if isinstance(place, int) else place
    return sum((place >= e).astype(jnp.int32) for e in ends[:-1])


def prompts(picked, raw, shares):
    tok, text = picked[0][0].shape[0], raw.shape[1]
    place = lax.broadcasted_iota(jnp.int32, (1, text), 1)
    for i, (queries, keys, _, _) in enumerate(picked):
        raw[pl.ds(i * tok, tok), :] = jnp.dot(queries, keys, preferred_element_type=jnp.float32)
    for i, (_, _, _, length) in enumerate(picked):
        for frame in range(tok // TPF):
            at = pl.ds(i * tok + frame * TPF, TPF)
            shares[at, :] = softmax(jnp.where(place < length, raw[at, :], -1e30))
    return [dot_last(shares[pl.ds(i * tok, tok), :], p[2]) for i, p in enumerate(picked)]


def early_kernel(chips, counts_ref, lengths_ref, tk_own, tv_own, tk_other, tv_other, *rest):
    early, tok = rest[-11].shape[:2]
    small, residual, blocks = rest[:3], rest[3], rest[4 : 4 + early]
    cross, tk, tv, *kept, own, other, raw, shares, sems = rest[4 + early :]
    videos, half = tk_own.shape[1:3]
    chip, core = my_chip(), my_core()
    sides = [residual.at[pl.ds(pl.multiple_of(c * (tok // 2), 16), tok // 2)] for c in (core, 1 - core)]
    copies = [
        pltpu.make_async_copy(source, target, sems.at[i])
        for i, (source, target) in enumerate(zip((*small, *sides), (*kept, own, other)))
    ]
    for copy in copies:
        copy.start()
    ends = video_ends(counts_ref)
    own_rows = pl.ds(pl.multiple_of(core * half, half), half)
    other_rows = pl.ds(pl.multiple_of((1 - core) * half, half), half)
    for video in range(videos):
        tk[video, own_rows, :] = tk_own[core, video]
        tk[video, other_rows, :] = tk_other[core, video]
        tv[video, own_rows, :] = tv_own[core, video]
        tv[video, other_rows, :] = tv_other[core, video]
    picked = []
    for index in range(early):
        video = video_of((chip ^ hop(index, chips)) * tok, ends)
        queries = blocks[index][pl.ds(0, tok), :]
        picked.append((queries, tk[video], tv[video], lengths_ref[core, video]))
    for index, out in enumerate(prompts(picked, raw, shares)):
        cross[index] = out
    for copy in copies:
        copy.wait()


def attend_kernel(chips, counts_ref, lengths_ref, tk, tv, early_ref, *rest):
    blocks, out_ref = rest[:chips], rest[chips]
    qs, ks, vs, cross, raw, weights, prompt_raw, shares = rest[chips + 1 :]
    tok = cross.shape[1]
    total = chips * tok
    strip = raw.shape[0]
    chip, core = my_chip(), my_core()
    ends = video_ends(counts_ref)
    for index in range(chips):
        h = chip ^ hop(index, chips)
        at = rows(h * tok, tok)
        for part, target in enumerate((qs, ks, vs)):
            target[at, :] = blocks[index][pl.ds(part * tok, tok), :]

    def pick(h, video):
        queries = qs[rows(h * tok, tok), :]
        return queries, tk[video], tv[video], lengths_ref[core, video]

    early = early_ref.shape[0]
    late = [chip ^ hop(index, chips) for index in range(early, chips)]
    begun = [ends[video - 1] // tok for video in range(1, len(ends))]
    picked = [pick(h, video_of(h * tok, ends)) for h in late]
    picked += [pick(h, video + 1) for video, h in enumerate(begun)]
    found = prompts(picked, prompt_raw, shares)
    for index in range(early):
        cross[chip ^ hop(index, chips)] = early_ref[index]
    for h, out in zip(late, found):
        cross[h] = out
    for video, (h, out) in enumerate(zip(begun, found[len(late) :])):
        for frame in range(tok // TPF):
            at = pl.ds(frame * TPF, TPF)
            here = video_of(h * tok + frame * TPF, ends) == video + 1
            cross[h, at, :] = jnp.where(here, out[frame * TPF : (frame + 1) * TPF], cross[h, at, :])

    key_video = video_of(lax.broadcasted_iota(jnp.int32, (1, total), 1), ends)

    def one_strip(index, carry):
        base = index * strip
        raw[...] = dot_last(qs[rows(base, strip), :], ks[...])
        for frame in range(strip // TPF):
            at = pl.ds(frame * TPF, TPF)
            allowed = key_video == video_of(base + frame * TPF, ends)
            weights[at, :] = softmax(jnp.where(allowed, raw[at, :], -1e30))
        out = jnp.dot(weights[...], vs[...], preferred_element_type=jnp.float32)
        for b in range(strip // tok):
            h = index * (strip // tok) + b
            whole = (out[b * tok : (b + 1) * tok] + cross[h]).astype(jnp.bfloat16)
            out_ref[place_of(h, chips)] = jnp.concatenate([whole[tok // 2 :], whole[: tok // 2]])
        return carry

    repeat(total // strip, one_strip)


def head_kernel(chips, scale_ref, x_ref, x_other, gain_ref, shift_ref, weight_ref, bias_ref, blocks, out_ref):
    _, width = x_ref.shape
    core = my_core()
    gain, shift = (ref[...].reshape(1, width) for ref in (gain_ref, shift_ref))

    def velocity(x, branch):
        attention = jnp.concatenate([blocks[2 * place_of(h, chips) + 1 - branch] for h in range(chips)], axis=-1)
        hidden = x.astype(jnp.float32) + attention.astype(jnp.float32)
        mean = jnp.sum(hidden, axis=-1, keepdims=True) * (1.0 / width)
        centred = hidden - mean
        var = jnp.sum(centred * centred, axis=-1, keepdims=True) * (1.0 / width)
        normed = centred * lax.rsqrt(var + 1e-06) * gain + shift
        return dot_last(normed.astype(jnp.bfloat16), weight_ref[...]) + bias_ref[...].reshape(1, -1)

    own, other = velocity(x_ref[...], core), velocity(x_other[...], 1 - core)
    scale = scale_ref[0]
    share = jnp.where(core == 0, scale, 1.0 - scale)
    out_ref[...] = other + share * (own - other)


def local(
    queries,
    self_keys,
    self_values,
    residual_in,
    text_keys,
    text_values,
    text_lengths,
    frame_counts,
    mod_gain,
    mod_shift,
    head_weight,
    head_bias,
    guide_scale,
):
    devices = lax.axis_size("seq")
    chips = devices // 2
    tok, width = queries.shape
    total = chips * tok
    bf16, f32 = jnp.bfloat16, jnp.float32
    block_shape = jax.ShapeDtypeStruct((3 * tok, HEAD_CHANNELS), bf16)
    text_keys = jnp.swapaxes(text_keys, 2, 3)
    text_values = jnp.swapaxes(text_values, 2, 3)
    vectors = (mod_gain, mod_shift, head_bias)
    packed = pl.pallas_call(
        functools.partial(pack_kernel, chips),
        out_shape=[block_shape] * chips,
        in_specs=[HBM] * 3,
        out_specs=[VMEM] * chips,
        scratch_shapes=[pltpu.SemaphoreType.DMA((3 * chips,))],
        compiler_params=params(8),
        name="pack",
    )(*(pltpu.with_memory_space_constraint(x, pltpu.HBM) for x in (queries, self_keys, self_values)))
    blocks = list(packed)
    for index in range(1, chips):
        blocks[index] = lax.ppermute(blocks[index], "seq", chip_pairs(devices, index))
    other_keys = lax.ppermute(text_keys, "seq", core_pairs(devices))
    other_values = lax.ppermute(text_values, "seq", core_pairs(devices))
    videos, half, text = text_keys.shape[1:]
    tokens = pltpu.VMEM((total, HEAD_CHANNELS), bf16)
    strip = math.gcd(chips, STRIP) * tok
    early = max(chips - LATE, 1)
    joined = jax.ShapeDtypeStruct((videos, 2 * half, text), bf16)
    cross, keys, values, *vectors, x_own, x_other = pl.pallas_call(
        functools.partial(early_kernel, chips),
        out_shape=[
            jax.ShapeDtypeStruct((early, tok, HEAD_CHANNELS), f32),
            joined,
            joined,
        ]
        + [jax.ShapeDtypeStruct(v.shape, v.dtype) for v in vectors]
        + [jax.ShapeDtypeStruct((tok // 2, width), bf16)] * 2,
        in_specs=[SMEM] * 2 + [VMEM] * 4 + [HBM] * 4 + [VMEM] * early,
        out_specs=[VMEM] * 8,
        scratch_shapes=[
            pltpu.VMEM((early * tok, text), f32),
            pltpu.VMEM((early * tok, text), bf16),
            pltpu.SemaphoreType.DMA((5,)),
        ],
        cost_estimate=pl.CostEstimate(
            flops=4 * early * tok * text * HEAD_CHANNELS,
            bytes_accessed=4 * total * HEAD_CHANNELS,
            transcendentals=early * tok * text,
        ),
        compiler_params=params(12),
        name="early",
    )(
        frame_counts,
        text_lengths,
        text_keys,
        text_values,
        other_keys,
        other_values,
        *(pltpu.with_memory_space_constraint(x, pltpu.HBM) for x in (*vectors, residual_in)),
        *blocks[:early],
    )
    x_other = lax.ppermute(x_other, "seq", core_pairs(devices))
    attended = pl.pallas_call(
        functools.partial(attend_kernel, chips),
        out_shape=jax.ShapeDtypeStruct((chips, tok, HEAD_CHANNELS), bf16),
        in_specs=[SMEM] * 2 + [VMEM] * (3 + chips),
        out_specs=VMEM,
        scratch_shapes=[tokens] * 3
        + [
            pltpu.VMEM((chips, tok, HEAD_CHANNELS), f32),
            pltpu.VMEM((strip, total), f32),
            pltpu.VMEM((strip, total), bf16),
            pltpu.VMEM(((chips - early + videos - 1) * tok, text), f32),
            pltpu.VMEM(((chips - early + videos - 1) * tok, text), bf16),
        ],
        cost_estimate=pl.CostEstimate(
            flops=4 * total * total * HEAD_CHANNELS,
            bytes_accessed=8 * total * HEAD_CHANNELS,
            transcendentals=total * total,
        ),
        compiler_params=params(24),
        name="attend",
    )(frame_counts, text_lengths, keys, values, cross, *blocks)
    returned = lax.all_to_all(
        attended.reshape(devices, tok // 2, HEAD_CHANNELS),
        "seq",
        split_axis=0,
        concat_axis=0,
        axis_index_groups=[[((d + 2 * lead(chips)) % devices) ^ 1 for d in range(devices)]],
        tiled=True,
    )

    return pl.pallas_call(
        functools.partial(head_kernel, chips),
        out_shape=jax.ShapeDtypeStruct((tok // 2, head_weight.shape[1]), f32),
        in_specs=[SMEM] + [VMEM] * 7,
        out_specs=VMEM,
        compiler_params=params(8),
        name="head",
    )(guide_scale, x_own, x_other, vectors[0], vectors[1], head_weight.T, vectors[2], returned)


def solution(mesh):
    return jax.shard_map(
        local,
        mesh=mesh,
        in_specs=(
            P(("parts", "seq"), None),
            P(("parts", "seq"), None),
            P(("parts", "seq"), None),
            P(("parts", "seq"), None),
            P(None, "parts", None, "seq"),
            P(None, "parts", None, "seq"),
            P(None, "parts"),
            P("parts"),
            P(),
            P(),
            P(),
            P(),
            P(),
        ),
        out_specs=P(("parts", "seq"), None),
        check_vma=False,
    )
```
